32 devices in a mesh: seq: 8 (over z, y), head: 4 (over x, core).
Axes of the slice: x: 2, y: 2, z: 4, core: 2. Of those that a mesh axis runs over, the one named last changes fastest.
Arguments:
- queries: float32 [1024, 8192], P('seq', 'head'), may hold values from -48 to 48
- prefix_keys: float32 [5120, 512], P('seq', 'head'), may hold values from -5 to 5
- prefix_value_rows: float32 [5120, 512], P('seq', 'head'), may hold values from -6 to 6
- response_keys: float32 [1024, 512], P('seq', 'head'), may hold values from -6 to 6
- response_values: float32 [1024, 512], P('seq', 'head'), may hold values from -6 to 6
- out_grad: float32 [1024, 8192], P('seq', 'head'), may hold values from -6 to 6
- lengths: int32 [8], P('seq'), may hold values from 32 to 128
Outputs:
- grad_queries: float32 [1024, 8192], P(('seq', 'head'))
- grad_prefix_keys: float32 [5120, 512], P('seq', 'head')
- grad_prefix_values: float32 [5120, 512], P('seq', 'head')
- grad_resp_keys: float32 [1024, 512], P('seq', 'head')
- grad_resp_values: float32 [1024, 512], P('seq', 'head')
The draws below stay inside these ranges and needn't reach their ends.
All inputs are finite; a program needn't handle non-finite values.
Results may differ from the reference program's by a relative error of at most 0.0003.
Values sent between devices are 32-bit elements; how exact they have to be, the bound alone decides.
A program may use at most 128 MiB of HBM per device.

```python
import jax
import jax.numpy as jnp
from jax import lax

QUERY_HEAD_COUNT = 64
KEY_VALUE_HEADS = 4
HEAD_SIZE = 128
BLOCK_PREFIX = 640
R_DEV = 128
WINDOW = 3
PREFIX_TOKENS = 5120
RESPONSE_SLOTS = 1024
N_SEQ = 8


def joint_draw(key):
    random_key_for_keys = jax.random.fold_in(key, 101)
    key_query = jax.random.fold_in(key, 202)
    key_matrix = jnp.clip(jax.random.normal(random_key_for_keys, (N_SEQ, BLOCK_PREFIX, KEY_VALUE_HEADS, HEAD_SIZE), jnp.float32), -4.0, 4.0)
    query_matrix = jnp.clip(jax.random.normal(key_query, (N_SEQ, R_DEV, QUERY_HEAD_COUNT, HEAD_SIZE), jnp.float32), -4.0, 4.0)
    return (key_matrix.reshape(PREFIX_TOKENS, KEY_VALUE_HEADS * HEAD_SIZE), query_matrix.reshape(RESPONSE_SLOTS, QUERY_HEAD_COUNT * HEAD_SIZE))


def draw_queries(key, part):
    return joint_draw(key)[1]


def draw_prefix_keys(key, part):
    return joint_draw(key)[0]


def set_ends(entries, key, low, high):
    place = [jax.random.randint(jax.random.fold_in(key, axis), (), 0, length) for axis, length in enumerate(entries.shape)]
    longest = entries.shape.index(max(entries.shape))
    next_to = place[:longest] + [(place[longest] + 1) % entries.shape[longest]] + place[longest + 1:]
    return entries.at[tuple(place)].set(low).at[tuple(next_to)].set(high)


def shard_levels(stream_key, dims, pieces, low, high):
    def one(position, shards_of):
        draws = jax.random.uniform(jax.random.fold_in(jax.random.fold_in(stream_key, 6), position), (shards_of,), jnp.float32, low / len(pieces), high / len(pieces))
        return jnp.repeat(jnp.exp(draws), dims[position] // shards_of).reshape((-1,) + (1,) * (len(dims) - position - 1))

    factor_of = one(*pieces[0])
    for cut in pieces[1:]:
        factor_of = factor_of * one(*cut)
    return factor_of


def bell_draw(stream_key, dims, width, bound, split=(), held_as=jnp.bfloat16):
    entries = jax.random.normal(stream_key, dims, jnp.float32) * width
    if len(split) > 0:
        entries = shard_levels(stream_key, dims, split, -0.22, 0.18) * entries
    return jnp.clip(entries, min=-bound, max=bound).astype(held_as)


def setup_inputs(seed: int = 0) -> dict:
    key_of = jax.random.split(jax.random.key(seed), 8)
    return {
        "queries": draw_queries(jax.random.fold_in(key_of[7], 71), 0),
        "prefix_keys": draw_prefix_keys(jax.random.fold_in(key_of[7], 71), 0),
        "prefix_value_rows": bell_draw(key_of[2], (PREFIX_TOKENS, KEY_VALUE_HEADS * HEAD_SIZE), 1.0, 6.0, ((0, 8), (1, 4)), jnp.float32),
        "response_keys": bell_draw(key_of[3], (RESPONSE_SLOTS, KEY_VALUE_HEADS * HEAD_SIZE), 1.0, 6.0, ((0, 8), (1, 4)), jnp.float32),
        "response_values": bell_draw(key_of[4], (RESPONSE_SLOTS, KEY_VALUE_HEADS * HEAD_SIZE), 1.0, 6.0, ((0, 8), (1, 4)), jnp.float32),
        "out_grad": bell_draw(key_of[5], (RESPONSE_SLOTS, QUERY_HEAD_COUNT * HEAD_SIZE), 1.0, 6.0, ((0, 8), (1, 4)), jnp.float32),
        "lengths": set_ends(jax.random.randint(key_of[6], (N_SEQ,), max(4, R_DEV // 4), R_DEV + 1), jax.random.fold_in(key_of[6], 1), max(4, R_DEV // 4), R_DEV).astype(jnp.int32),
    }


def attend(query_row_block, visible_key_rows, visible_value_rows, local_block_keys, local_block_values, length):
    row_count = query_row_block.shape[0]
    group_size = QUERY_HEAD_COUNT // KEY_VALUE_HEADS
    prefix_length = visible_key_rows.shape[0]
    query_block = query_row_block.reshape(row_count, KEY_VALUE_HEADS, group_size, HEAD_SIZE)
    key_matrix = jnp.concatenate([visible_key_rows, local_block_keys], axis=0).reshape(prefix_length + row_count, KEY_VALUE_HEADS, HEAD_SIZE)
    value_matrix = jnp.concatenate([visible_value_rows, local_block_values], axis=0).reshape(prefix_length + row_count, KEY_VALUE_HEADS, HEAD_SIZE)
    scores = jnp.einsum('rkgd,skd->kgrs', query_block, key_matrix, precision=lax.Precision.HIGHEST) * HEAD_SIZE ** (-0.5)
    slot = jnp.arange(prefix_length + row_count, dtype=jnp.int32) - prefix_length
    token = jnp.arange(row_count, dtype=jnp.int32)
    visible = (slot[None, :] < 0) | (slot[None, :] <= token[:, None]) & (slot[None, :] < length)
    scores = jnp.where(visible[None, None], scores, -1e+30)
    probs = jax.nn.softmax(scores, axis=-1)
    result = jnp.einsum('kgrs,skd->rkgd', probs, value_matrix, precision=lax.Precision.HIGHEST)
    return result.reshape(row_count, QUERY_HEAD_COUNT * HEAD_SIZE)

def reference(queries, prefix_keys, prefix_value_rows, response_keys, response_values, out_grad, lengths):
    window_width = KEY_VALUE_HEADS * HEAD_SIZE
    q_blocks = queries.reshape(N_SEQ, R_DEV, QUERY_HEAD_COUNT * HEAD_SIZE)
    g_blocks = out_grad.reshape(N_SEQ, R_DEV, QUERY_HEAD_COUNT * HEAD_SIZE)
    kp_blocks = prefix_keys.reshape(N_SEQ, BLOCK_PREFIX, window_width)
    vp_blocks = prefix_value_rows.reshape(N_SEQ, BLOCK_PREFIX, window_width)
    kr_blocks = response_keys.reshape(N_SEQ, R_DEV, window_width)
    vr_blocks = response_values.reshape(N_SEQ, R_DEV, window_width)

    def one_response(index):
        picks = (index + jnp.arange(WINDOW, dtype=jnp.int32)) % N_SEQ
        visible_key_rows = jnp.take(kp_blocks, picks, axis=0).reshape(WINDOW * BLOCK_PREFIX, window_width)
        visible_value_rows = jnp.take(vp_blocks, picks, axis=0).reshape(WINDOW * BLOCK_PREFIX, window_width)
        length = lengths[index]
        valid = (jnp.arange(R_DEV, dtype=jnp.int32) < length).astype(jnp.float32)

        def forward(a, b, c, d, e):
            return attend(a, b, c, d, e, length)
        _, pullback = jax.vjp(forward, q_blocks[index], visible_key_rows, visible_value_rows, kr_blocks[index], vr_blocks[index])
        dq, dkw, dvw, dkr, dvr = pullback(g_blocks[index] * valid[:, None])
        return (dq, dkw.reshape(WINDOW, BLOCK_PREFIX, window_width), dvw.reshape(WINDOW, BLOCK_PREFIX, window_width), dkr, dvr)
    dq, dkw, dvw, dkr, dvr = lax.map(one_response, jnp.arange(N_SEQ, dtype=jnp.int32))
    grad_k = dkw[:, 0]
    grad_v = dvw[:, 0]
    for offset in range(1, WINDOW):
        grad_k = grad_k + jnp.roll(dkw[:, offset], offset, axis=0)
        grad_v = grad_v + jnp.roll(dvw[:, offset], offset, axis=0)
    return (dq.reshape(RESPONSE_SLOTS, QUERY_HEAD_COUNT * HEAD_SIZE), grad_k.reshape(PREFIX_TOKENS, window_width), grad_v.reshape(PREFIX_TOKENS, window_width), dkr.reshape(RESPONSE_SLOTS, window_width), dvr.reshape(RESPONSE_SLOTS, window_width))
```

```python
import functools
import math

import jax
import jax.numpy as jnp
from jax import lax
from jax.experimental import pallas as pl
from jax.experimental.pallas import tpu as pltpu
from jax.sharding import PartitionSpec as P

HEAD_SIZE = 128
WINDOW = 3
D = HEAD_SIZE
MESH = pl.DeviceIdType.MESH
F32, BF16 = jnp.float32, jnp.bfloat16
CHUNKS = 2
SUB = 128


def split(x):
    hi = x.astype(BF16)
    lo = (x - hi.astype(F32)).astype(BF16)
    return hi, lo


def dot(a, b):
    return jnp.dot(a, b, preferred_element_type=F32)


def kernel(
    n_seq, n_head,
    length_ref, q_ref, pk_ref, pv_ref, rk_ref, rv_ref, g_ref,
    gq_ref, gpk_ref, gpv_ref, grk_ref, grv_ref,
    kv1, kv2, kc, vc, kt, qt, gt, qr, gr, s_ref, dp_ref, m_ref, l_ref, d_ref,
    pcat, dcat, dk_acc, dv_acc, dqt, dqs, ry, rz,
    in_z_send, in_z_recv, in_y_send, in_y_recv,
    out_z_send, out_z_recv, out_y_send, out_y_recv,
    q_send, q_recv, q_local,
):
    rows = q_ref.shape[0]
    heads = q_ref.shape[1] // D
    pairs = heads // 2
    block = pk_ref.shape[0]
    piece = block // CHUNKS
    lead = block + rows
    off1, off2 = lead, lead + block
    factor = D ** (-0.5)
    seq = lax.axis_index("seq")
    head = lax.axis_index("head")
    even = lax.rem(seq, 2) == 0
    partner = seq + 1 - 2 * lax.rem(seq, 2)
    below = lax.rem(seq + n_seq - 2, n_seq)
    above = lax.rem(seq + 2, n_seq)

    barrier = pltpu.get_barrier_semaphore()
    for other in (partner, below, above):
        pl.semaphore_signal(barrier, inc=1, device_id=(other, head), device_id_type=MESH)
    for step in range(1, n_head):
        pl.semaphore_signal(
            barrier, inc=1, device_id=(seq, lax.rem(head + step, n_head)), device_id_type=MESH
        )
    pl.semaphore_wait(barrier, 3 + n_head - 1)

    def remote(src, dst, send, recv, to):
        return pltpu.make_async_remote_copy(
            src_ref=src, dst_ref=dst, send_sem=send, recv_sem=recv,
            device_id=to, device_id_type=MESH,
        )

    pieces = [(c, t) for c in range(CHUNKS) for t in range(2)]
    own = (pk_ref, pv_ref)

    def at(c):
        return pl.ds(c * piece, piece)

    def in_z(c, t):
        return remote(own[t].at[at(c)], kv2.at[t, at(c)], in_z_send.at[c, t], in_z_recv.at[c, t], (below, head))

    def in_y_own(c, t):
        return remote(own[t].at[at(c)], kv1.at[t, at(c)], in_y_send.at[c, t], in_y_recv.at[c, t], (partner, head))

    def in_y_pass(c, t):
        return remote(kv2.at[t, at(c)], kv1.at[t, at(c)], in_y_send.at[c, t], in_y_recv.at[c, t], (partner, head))

    for c, t in pieces:
        in_z(c, t).start()

    @pl.when(jnp.logical_not(even))
    def _():
        for c, t in pieces:
            in_y_own(c, t).start()

    length = length_ref[0]
    token = lax.broadcasted_iota(jnp.int32, (rows, 1), 0)
    live = token < length
    for h in range(heads):
        cols = pl.ds(h * D, D)
        pair, half = h // 2, h % 2
        lanes = pl.ds(half * rows, rows)
        q = q_ref[:, cols]
        g = jnp.where(live, g_ref[:, cols], 0.0)
        for x, wide, tall, scale in (
            (q, qr, qt, factor * math.log2(math.e)),
            (g, gr, gt, 1.0),
        ):
            hi, lo = split((x * scale).T)
            tall[pair, 0:D, lanes] = hi
            tall[pair, D : 2 * D, lanes] = hi
            tall[pair, 2 * D : 3 * D, lanes] = lo
            hi, lo = split(x * factor) if wide is qr else split(x)
            for copy in range(2):
                at_rows = pl.ds(copy * 2 * rows + half * rows, rows)
                wide[pair, at_rows, 0:D] = hi
                wide[pair, at_rows, D : 2 * D] = lo

    def place(keys, values, offset, size):
        for start in range(0, size, SUB):
            here = pl.ds(offset + start, SUB)
            k = keys[pl.ds(start, SUB), :]
            hi, lo = split(k)
            kc[here, 0:D] = hi
            kc[here, D : 2 * D] = lo
            kc[here, 2 * D : 3 * D] = hi
            hi, lo = split(k.T)
            kt[0:D, here] = hi
            kt[D : 2 * D, here] = lo
            hi, lo = split(values[pl.ds(start, SUB), :])
            vc[here, 0:D] = hi
            vc[here, D : 2 * D] = lo
            vc[here, 2 * D : 3 * D] = hi

    def scores(offset, size, first):
        def body(pair, carry):
            s = dot(kc[pl.ds(offset, size), :], qt[pair])
            if first:
                slot = lax.broadcasted_iota(jnp.int32, (rows, 2 * rows), 0)
                lane = lax.broadcasted_iota(jnp.int32, (rows, 2 * rows), 1)
                query = jnp.where(lane >= rows, lane - rows, lane)
                visible = (slot <= query) & (slot < length)
                s_ref[pair, pl.ds(offset, block), :] = s[:block]
                s_ref[pair, pl.ds(offset + block, rows), :] = jnp.where(visible, s[block:], -1e30)
            else:
                s_ref[pair, pl.ds(offset, size), :] = s
            dp_ref[pair, pl.ds(offset, size), :] = dot(vc[pl.ds(offset, size), :], gt[pair])
            top = None
            for start in range(0, size, SUB):
                part = jnp.max(
                    s_ref[pair, pl.ds(offset + start, SUB), :].reshape(SUB // 8, 8, 2 * rows), axis=0
                )
                top = part if top is None else jnp.maximum(top, part)
            top = jnp.max(top, axis=0, keepdims=True)
            total = jnp.zeros((8, 2 * rows), F32)
            dsum = jnp.zeros((8, 2 * rows), F32)
            for start in range(0, size, SUB):
                here = pl.ds(offset + start, SUB)
                e = jnp.exp2(s_ref[pair, here, :] - top)
                total = total + jnp.sum(e.reshape(SUB // 8, 8, 2 * rows), axis=0)
                dsum = dsum + jnp.sum((e * dp_ref[pair, here, :]).reshape(SUB // 8, 8, 2 * rows), axis=0)
            total = jnp.sum(total, axis=0, keepdims=True)
            dsum = jnp.sum(dsum, axis=0, keepdims=True)
            if first:
                m_ref[pair] = top
                l_ref[pair] = total
                d_ref[pair] = dsum
            else:
                newest = jnp.maximum(m_ref[pair], top)
                fade, add = jnp.exp2(m_ref[pair] - newest), jnp.exp2(top - newest)
                m_ref[pair] = newest
                l_ref[pair] = l_ref[pair] * fade + total * add
                d_ref[pair] = d_ref[pair] * fade + dsum * add
            return carry

        lax.fori_loop(0, pairs, body, 0)

    def grads(offset, size, first):
        keys = pl.ds(offset, size)
        dk_acc[keys, :] = jnp.zeros((size, D), F32)
        dv_acc[keys, :] = jnp.zeros((size, D), F32)

        def body(pair, carry):
            shift, mean = m_ref[pair], d_ref[pair]
            for start in range(0, size, SUB):
                here = pl.ds(offset + start, SUB)
                p = jnp.exp2(s_ref[pair, here, :] - shift)
                ds = p * (dp_ref[pair, here, :] - mean)
                to = pl.ds(start, SUB)
                hi, lo = split(p)
                pcat[to, 0 : 2 * rows] = hi
                pcat[to, 2 * rows :] = lo
                hi, lo = split(ds)
                dcat[to, 0 : 2 * rows] = hi
                dcat[to, 2 * rows :] = lo
            some = pl.ds(0, size)
            dv = dot(pcat[some, :], gr[pair])
            dv_acc[keys, :] += dv[:, :D] + dv[:, D:]
            dk = dot(dcat[some, :], qr[pair])
            dk_acc[keys, :] += dk[:, :D] + dk[:, D:]
            high = dot(kt[:, keys], dcat[some, 0 : 2 * rows])
            dq = high[:D] + high[D:] + dot(kt[0:D, keys], dcat[some, 2 * rows :])
            if first:
                dqt[pair] = dq
            else:
                dqt[pair] += dq
            return carry

        lax.fori_loop(0, pairs, body, 0)

    place(pk_ref, pv_ref, 0, block)
    place(rk_ref, rv_ref, block, rows)
    scores(0, lead, True)

    for c, t in pieces:
        in_z(c, t).wait_recv()

        @pl.when(even)
        def _():
            in_y_pass(c, t).start()

    place(kv2.at[0], kv2.at[1], off2, block)
    scores(off2, block, False)
    for c, t in pieces:
        in_y_own(c, t).wait_recv()
    place(kv1.at[0], kv1.at[1], off1, block)
    scores(off1, block, False)

    def finish(pair, carry):
        l = l_ref[pair]
        d_ref[pair] = d_ref[pair] / l
        m_ref[pair] = m_ref[pair] + jnp.log2(l)
        return carry

    lax.fori_loop(0, pairs, finish, 0)

    acc = (dk_acc, dv_acc)

    def out_y(c, t):
        return remote(
            acc[t].at[pl.ds(off1 + c * piece, piece)], ry.at[t, at(c)],
            out_y_send.at[c, t], out_y_recv.at[c, t], (partner, head),
        )

    def out_z(c, t):
        return remote(
            acc[t].at[pl.ds(off2 + c * piece, piece)], rz.at[t, at(c)],
            out_z_send.at[c, t], out_z_recv.at[c, t], (above, head),
        )

    grads(off1, block, True)
    for c, t in pieces:
        out_y(c, t).start()
    grads(off2, block, False)

    @pl.when(jnp.logical_not(even))
    def _():
        for c, t in pieces:
            out_z(c, t).start()

    grads(0, lead, False)
    grk_ref[...] = dk_acc[pl.ds(block, rows), :]
    grv_ref[...] = dv_acc[pl.ds(block, rows), :]

    for h in range(heads):
        dqs[:, pl.ds(h * D, D)] = dqt[h // 2, :, pl.ds(h % 2 * rows, rows)].T * factor

    width = heads * D
    share = rows // n_head

    def to_peer(step):
        other = lax.rem(head + step, n_head)
        return remote(
            dqs.at[pl.ds(other * share, share), :],
            gq_ref.at[:, pl.ds(pl.multiple_of(head * width, D), width)],
            q_send.at[step - 1], q_recv.at[step - 1], (seq, other),
        )

    keep = pltpu.make_async_copy(
        dqs.at[pl.ds(head * share, share), :],
        gq_ref.at[:, pl.ds(pl.multiple_of(head * width, D), width)],
        q_local,
    )
    for step in range(1, n_head):
        to_peer(step).start()
    keep.start()

    for c, t in pieces:
        out_y(c, t).wait_recv()

        @pl.when(even)
        def _():
            acc[t][pl.ds(off2 + c * piece, piece), :] += ry[t, at(c), :]
            out_z(c, t).start()

        @pl.when(jnp.logical_not(even))
        def _():
            acc[t][pl.ds(c * piece, piece), :] += ry[t, at(c), :]

    out = (gpk_ref, gpv_ref)
    for c, t in pieces:
        out_z(c, t).wait_recv()
        out[t][at(c), :] = acc[t][at(c), :] + rz[t, at(c), :]

    keep.wait()
    for step in range(1, n_head):
        to_peer(step).wait()
    for c, t in pieces:
        in_z(c, t).wait_send()
        in_y_own(c, t).wait_send()
        out_y(c, t).wait_send()
        out_z(c, t).wait_send()


def per_device(n_seq, n_head, queries, prefix_keys, prefix_value_rows, response_keys, response_values, out_grad, lengths):
    rows, width = queries.shape
    block = prefix_keys.shape[0]
    assert prefix_keys.shape[1] == D
    heads = width // D
    pairs = heads // 2
    keys = WINDOW * block + rows
    lead = block + rows
    vmem = pl.BlockSpec(memory_space=pltpu.VMEM)
    sems = pltpu.SemaphoreType.DMA((CHUNKS, 2))
    shape = jax.ShapeDtypeStruct
    return pl.pallas_call(
        functools.partial(kernel, n_seq, n_head),
        out_shape=(
            shape((rows // n_head, width * n_head), F32),
            shape((block, D), F32),
            shape((block, D), F32),
            shape((rows, D), F32),
            shape((rows, D), F32),
        ),
        in_specs=[pl.BlockSpec(memory_space=pltpu.SMEM)] + [vmem] * 6,
        out_specs=(pl.BlockSpec(memory_space=pl.ANY), vmem, vmem, vmem, vmem),
        scratch_shapes=[
            pltpu.VMEM((2, block, D), F32),
            pltpu.VMEM((2, block, D), F32),
            pltpu.VMEM((keys, 3 * D), BF16),
            pltpu.VMEM((keys, 3 * D), BF16),
            pltpu.VMEM((2 * D, keys), BF16),
            pltpu.VMEM((pairs, 3 * D, 2 * rows), BF16),
            pltpu.VMEM((pairs, 3 * D, 2 * rows), BF16),
            pltpu.VMEM((pairs, 4 * rows, 2 * D), BF16),
            pltpu.VMEM((pairs, 4 * rows, 2 * D), BF16),
            pltpu.VMEM((pairs, keys, 2 * rows), F32),
            pltpu.VMEM((pairs, keys, 2 * rows), F32),
            pltpu.VMEM((pairs, 1, 2 * rows), F32),
            pltpu.VMEM((pairs, 1, 2 * rows), F32),
            pltpu.VMEM((pairs, 1, 2 * rows), F32),
            pltpu.VMEM((lead, 4 * rows), BF16),
            pltpu.VMEM((lead, 4 * rows), BF16),
            pltpu.VMEM((keys, D), F32),
            pltpu.VMEM((keys, D), F32),
            pltpu.VMEM((pairs, D, 2 * rows), F32),
            pltpu.VMEM((rows, width), F32),
            pltpu.VMEM((2, block, D), F32),
            pltpu.VMEM((2, block, D), F32),
        ]
        + [sems] * 8
        + [pltpu.SemaphoreType.DMA((n_head - 1,))] * 2
        + [pltpu.SemaphoreType.DMA],
        compiler_params=pltpu.CompilerParams(
            collective_id=0, has_side_effects=True, vmem_limit_bytes=63 * 1024 * 1024
        ),
    )(lengths, queries, prefix_keys, prefix_value_rows, response_keys, response_values, out_grad)


def solution(mesh):
    sharded = P("seq", "head")
    return jax.shard_map(
        functools.partial(per_device, mesh.shape["seq"], mesh.shape["head"]),
        mesh=mesh,
        in_specs=(sharded,) * 6 + (P("seq"),),
        out_specs=(P(("seq", "head"), None),) + (sharded,) * 4,
        check_vma=False,
    )
```

```python
import functools
import math

import jax
import jax.numpy as jnp
from jax import lax
from jax.experimental import pallas as pl
from jax.experimental.pallas import tpu as pltpu
from jax.sharding import PartitionSpec as P

HEAD_SIZE = 128
WINDOW = 3
D = HEAD_SIZE
MESH = pl.DeviceIdType.MESH
F32, BF16 = jnp.float32, jnp.bfloat16
SUB = 128
UNROLL = 4


def split(x):
    hi = x.astype(BF16)
    lo = (x - hi.astype(F32)).astype(BF16)
    return hi, lo


def dot(a, b):
    return jnp.dot(a, b, preferred_element_type=F32)


def chunk_of(block):
    return (block // SUB + 1) // 2 * SUB


def kernel(
    n_seq, n_head,
    length_ref, q_hbm, pk_ref, pv_ref, rk_ref, rv_ref, g_hbm,
    gq_ref, gpk_ref, gpv_ref, grk_ref, grv_ref,
    q_ref, g_ref, kv0, kv1, kv2, kvr, kc, vc, kt, qt, gt, qr, gr, s_ref, dp_ref, m_ref, l_ref, d_ref,
    pcat, dcat, dk_acc, dv_acc, dqt, dqs, ry, rz,
    in_z_send, in_z_recv, in_y_send, in_y_recv,
    out_z_send, out_z_recv, out_y_send, out_y_recv,
    q_send, q_recv, q_local, load_sem,
):
    rows = q_hbm.shape[0]
    heads = q_hbm.shape[1] // D
    pairs = heads // 2
    block = pk_ref.shape[0]
    big = chunk_of(block)
    spans = ((0, big), (big, block - big))
    lead = block + rows
    off1, off2 = lead, lead + block
    factor = D ** (-0.5)
    seq = lax.axis_index("seq")
    head = lax.axis_index("head")
    even = lax.rem(seq, 2) == 0
    odd = jnp.logical_not(even)
    partner = seq + 1 - 2 * lax.rem(seq, 2)
    below = lax.rem(seq + n_seq - 2, n_seq)
    above = lax.rem(seq + 2, n_seq)

    barrier = pltpu.get_barrier_semaphore()
    for other in (partner, below, above):
        pl.semaphore_signal(barrier, inc=1, device_id=(other, head), device_id_type=MESH)
    for step in range(1, n_head):
        pl.semaphore_signal(
            barrier, inc=1, device_id=(seq, lax.rem(head + step, n_head)), device_id_type=MESH
        )
    loads = [
        pltpu.make_async_copy(src, dst, load_sem.at[i])
        for i, (src, dst) in enumerate(
            (
                (pk_ref, kv0.at[0]),
                (pv_ref, kv0.at[1]),
                (rk_ref, kvr.at[0]),
                (rv_ref, kvr.at[1]),
                (q_hbm, q_ref),
                (g_hbm, g_ref),
            )
        )
    ]
    for load in loads:
        load.start()
    pl.semaphore_wait(barrier, 3 + n_head - 1)

    def remote(src, dst, send, recv, to):
        return pltpu.make_async_remote_copy(
            src_ref=src, dst_ref=dst, send_sem=send, recv_sem=recv,
            device_id=to, device_id_type=MESH,
        )

    pieces = [(c, t) for c in range(2) for t in range(2)]
    own = (pk_ref, pv_ref)

    def at(c):
        return pl.ds(*spans[c])

    def in_z(c, t):
        return remote(own[t].at[at(c)], kv2.at[t, at(c)], in_z_send.at[c, t], in_z_recv.at[c, t], (below, head))

    def in_y_own(c, t):
        return remote(own[t].at[at(c)], kv1.at[t, at(c)], in_y_send.at[c, t], in_y_recv.at[c, t], (partner, head))

    def in_y_pass(c, t):
        return remote(kv2.at[t, at(c)], kv1.at[t, at(c)], in_y_send.at[c, t], in_y_recv.at[c, t], (partner, head))

    for c, t in pieces:
        in_z(c, t).start()

    @pl.when(odd)
    def _():
        for c, t in pieces:
            in_y_own(c, t).start()

    def place(keys, values, first, offset, size):
        for start in range(0, size, SUB):
            here = pl.ds(offset + start, SUB)
            k = keys[pl.ds(first + start, SUB), :]
            hi, lo = split(k)
            kc[here, 0:D] = hi
            kc[here, D : 2 * D] = lo
            kc[here, 2 * D : 3 * D] = hi
            hi, lo = split(k.T)
            kt[0:D, here] = hi
            kt[D : 2 * D, here] = lo
            hi, lo = split(values[pl.ds(first + start, SUB), :])
            vc[here, 0:D] = hi
            vc[here, D : 2 * D] = lo
            vc[here, 2 * D : 3 * D] = hi

    for load in loads[:4]:
        load.wait()
    place(kv0.at[0], kv0.at[1], 0, 0, block)
    place(kvr.at[0], kvr.at[1], 0, block, rows)
    for load in loads[4:]:
        load.wait()

    length = length_ref[0]
    token = lax.broadcasted_iota(jnp.int32, (rows, 1), 0)
    live = token < length
    for h in range(heads):
        cols = pl.ds(h * D, D)
        pair, half = h // 2, h % 2
        lanes = pl.ds(half * rows, rows)
        q = q_ref[:, cols]
        g = jnp.where(live, g_ref[:, cols], 0.0)
        for x, wide, tall, scale in (
            (q, qr, qt, factor * math.log2(math.e)),
            (g, gr, gt, 1.0),
        ):
            hi, lo = split((x * scale).T)
            tall[pair, 0:D, lanes] = hi
            tall[pair, D : 2 * D, lanes] = hi
            tall[pair, 2 * D : 3 * D, lanes] = lo
            hi, lo = split(x * factor) if wide is qr else split(x)
            for copy in range(2):
                at_rows = pl.ds(copy * 2 * rows + half * rows, rows)
                wide[pair, at_rows, 0:D] = hi
                wide[pair, at_rows, D : 2 * D] = lo

    def scores(offset, size, first):
        def products(pair):
            s = dot(kc[pl.ds(offset, size), :], qt[pair])
            if first:
                slot = lax.broadcasted_iota(jnp.int32, (rows, 2 * rows), 0)
                lane = lax.broadcasted_iota(jnp.int32, (rows, 2 * rows), 1)
                query = jnp.where(lane >= rows, lane - rows, lane)
                visible = (slot <= query) & (slot < length)
                s_ref[pair, pl.ds(offset, block), :] = s[:block]
                s_ref[pair, pl.ds(offset + block, rows), :] = jnp.where(visible, s[block:], -1e30)
            else:
                s_ref[pair, pl.ds(offset, size), :] = s
            dp_ref[pair, pl.ds(offset, size), :] = dot(vc[pl.ds(offset, size), :], gt[pair])

        def sums(pair):
            top = None
            for start in range(0, size, SUB):
                part = jnp.max(
                    s_ref[pair, pl.ds(offset + start, SUB), :].reshape(SUB // 8, 8, 2 * rows), axis=0
                )
                top = part if top is None else jnp.maximum(top, part)
            top = jnp.max(top, axis=0, keepdims=True)
            total = jnp.zeros((8, 2 * rows), F32)
            dsum = jnp.zeros((8, 2 * rows), F32)
            for start in range(0, size, SUB):
                here = pl.ds(offset + start, SUB)
                e = jnp.exp2(s_ref[pair, here, :] - top)
                total = total + jnp.sum(e.reshape(SUB // 8, 8, 2 * rows), axis=0)
                dsum = dsum + jnp.sum((e * dp_ref[pair, here, :]).reshape(SUB // 8, 8, 2 * rows), axis=0)
            total = jnp.sum(total, axis=0, keepdims=True)
            dsum = jnp.sum(dsum, axis=0, keepdims=True)
            if first:
                m_ref[pair] = top
                l_ref[pair] = total
                d_ref[pair] = dsum
            else:
                newest = jnp.maximum(m_ref[pair], top)
                fade, add = jnp.exp2(m_ref[pair] - newest), jnp.exp2(top - newest)
                m_ref[pair] = newest
                l_ref[pair] = l_ref[pair] * fade + total * add
                d_ref[pair] = d_ref[pair] * fade + dsum * add

        def body(i, carry):
            for j in range(UNROLL):
                products(i * UNROLL + j)
                if j:
                    sums(i * UNROLL + j - 1)
            sums(i * UNROLL + UNROLL - 1)
            return carry

        lax.fori_loop(0, pairs // UNROLL, body, 0)

    def grads(offset, size, first, begin=0, end=None, then=None):
        keys = pl.ds(offset, size)
        if begin == 0:
            dk_acc[keys, :] = jnp.zeros((size, D), F32)
            dv_acc[keys, :] = jnp.zeros((size, D), F32)
        some = pl.ds(0, size)

        def weights(pair, slot):
            shift, mean = m_ref[pair], d_ref[pair]
            for start in range(0, size, SUB):
                here = pl.ds(offset + start, SUB)
                p = jnp.exp2(s_ref[pair, here, :] - shift)
                ds = p * (dp_ref[pair, here, :] - mean)
                to = pl.ds(start, SUB)
                hi, lo = split(p)
                pcat[slot, to, 0 : 2 * rows] = hi
                pcat[slot, to, 2 * rows :] = lo
                hi, lo = split(ds)
                dcat[slot, to, 0 : 2 * rows] = hi
                dcat[slot, to, 2 * rows :] = lo

        def products(pair, slot):
            dv = dot(pcat[slot, some, :], gr[pair])
            dv_acc[keys, :] += dv[:, :D] + dv[:, D:]
            dk = dot(dcat[slot, some, :], qr[pair])
            dk_acc[keys, :] += dk[:, :D] + dk[:, D:]
            high = dot(kt[:, keys], dcat[slot, some, 0 : 2 * rows])
            dq = high[:D] + high[D:] + dot(kt[0:D, keys], dcat[slot, some, 2 * rows :])
            if first:
                dqt[pair] = dq
            elif then is None:
                dqt[pair] += dq
            else:
                then(pair, dqt[pair] + dq)

        def body(i, carry):
            weights(2 * i, 0)
            weights(2 * i + 1, 1)
            products(2 * i, 0)
            products(2 * i + 1, 1)
            return carry

        lax.fori_loop(begin // 2, (pairs if end is None else end) // 2, body, 0)

    scores(0, lead, True)
    for c in range(2):
        for t in range(2):
            in_z(c, t).wait_recv()

            @pl.when(even)
            def _():
                in_y_pass(c, t).start()

        place(kv2.at[0], kv2.at[1], spans[c][0], off2 + spans[c][0], spans[c][1])
        scores(off2 + spans[c][0], spans[c][1], False)
        for t in range(2):
            in_y_own(c, t).wait_recv()
        place(kv1.at[0], kv1.at[1], spans[c][0], off1 + spans[c][0], spans[c][1])
        scores(off1 + spans[c][0], spans[c][1], False)

    def finish(pair, carry):
        l = l_ref[pair]
        d_ref[pair] = d_ref[pair] / l
        m_ref[pair] = m_ref[pair] + jnp.log2(l)
        return carry

    lax.fori_loop(0, pairs, finish, 0)

    acc = (dk_acc, dv_acc)
    parts = block // SUB
    order = list(range(spans[1][0] // SUB, parts)) + list(range(spans[1][0] // SUB))
    split_at = spans[1][1] // SUB

    def out_y(i, t):
        return remote(
            acc[t].at[pl.ds(off1 + i * SUB, SUB)], ry.at[t, pl.ds(i * SUB, SUB)],
            out_y_send.at[i, t], out_y_recv.at[i, t], (partner, head),
        )

    def out_z(i, t):
        return remote(
            acc[t].at[pl.ds(off2 + i * SUB, SUB)], rz.at[t, pl.ds(i * SUB, SUB)],
            out_z_send.at[i, t], out_z_recv.at[i, t], (above, head),
        )

    def send_y(some):
        for i in some:
            for t in range(2):
                out_y(i, t).start()

    def send_z_odd(some):
        @pl.when(odd)
        def _():
            for i in some:
                for t in range(2):
                    out_z(i, t).start()

    def join(some):
        for i in some:
            for t in range(2):
                out_y(i, t).wait_recv()

            @pl.when(even)
            def _():
                for t in range(2):
                    acc[t][pl.ds(off2 + i * SUB, SUB), :] += ry[t, pl.ds(i * SUB, SUB), :]
                for t in range(2):
                    out_z(i, t).start()

    width = heads * D
    share = rows // n_head

    def to_peer(step, pair):
        other = lax.rem(head + step, n_head)
        return remote(
            dqs.at[pair, pl.ds(other * share, share), :],
            gq_ref.at[:, pl.ds(pl.multiple_of(head * width + pair * 2 * D, D), 2 * D)],
            q_send.at[step - 1, pair], q_recv.at[step - 1, pair], (seq, other),
        )

    def keep(pair):
        return pltpu.make_async_copy(
            dqs.at[pair, pl.ds(head * share, share), :],
            gq_ref.at[:, pl.ds(pl.multiple_of(head * width + pair * 2 * D, D), 2 * D)],
            q_local.at[pair],
        )

    def stage(pair, dq):
        for half in range(2):
            dqs[pair, :, half * D : (half + 1) * D] = dq[:, half * rows : (half + 1) * rows].T * factor
        for step in range(1, n_head):
            to_peer(step, pair).start()
        keep(pair).start()

    last, front = spans[1], spans[0]
    grads(off1 + last[0], last[1], True)
    send_y(order[:split_at])
    grads(off2 + last[0], last[1], False)
    send_z_odd(order[:split_at])
    grads(off1 + front[0], front[1], False)
    send_y(order[split_at:])
    join(order[:1])
    grads(off2 + front[0], front[1], False)
    send_z_odd(order[split_at:])
    join(order[1:split_at])
    middle = pairs // 4 * 2
    grads(0, lead, False, 0, middle, stage)
    join(order[split_at : split_at + 1])
    grads(0, lead, False, middle, pairs, stage)
    grk_ref[...] = dk_acc[pl.ds(block, rows), :]
    grv_ref[...] = dv_acc[pl.ds(block, rows), :]
    join(order[split_at + 1 :])

    @pl.when(odd)
    def _():
        for t in range(2):
            acc[t][pl.ds(0, block), :] += ry[t]

    out = (gpk_ref, gpv_ref)
    for i in order:
        for t in range(2):
            here = pl.ds(i * SUB, SUB)
            out_z(i, t).wait_recv()
            out[t][here, :] = acc[t][here, :] + rz[t, here, :]

    for pair in range(pairs):
        keep(pair).wait()
        for step in range(1, n_head):
            to_peer(step, pair).wait()
    for c, t in pieces:
        in_z(c, t).wait_send()
        in_y_own(c, t).wait_send()
    for i in order:
        for t in range(2):
            out_y(i, t).wait_send()
            out_z(i, t).wait_send()


def settle(*refs):
    count = len(refs) // 2
    sem = refs[-1]
    copies = [
        pltpu.make_async_copy(refs[i], refs[count + i], sem.at[i]) for i in range(count)
    ]
    for copy in copies:
        copy.start()
    for copy in copies:
        copy.wait()


def per_device(n_seq, n_head, queries, prefix_keys, prefix_value_rows, response_keys, response_values, out_grad, lengths):
    rows, width = queries.shape
    block = prefix_keys.shape[0]
    assert prefix_keys.shape[1] == D
    heads = width // D
    pairs = heads // 2
    keys = WINDOW * block + rows
    lead = block + rows
    vmem = pl.BlockSpec(memory_space=pltpu.VMEM)
    anywhere = pl.BlockSpec(memory_space=pl.ANY)
    sems = pltpu.SemaphoreType.DMA((2, 2))
    part_sems = pltpu.SemaphoreType.DMA((block // SUB, 2))
    shape = jax.ShapeDtypeStruct
    results = pl.pallas_call(
        functools.partial(kernel, n_seq, n_head),
        out_shape=(
            shape((rows // n_head, width * n_head), F32),
            shape((block, D), F32),
            shape((block, D), F32),
            shape((rows, D), F32),
            shape((rows, D), F32),
        ),
        in_specs=[pl.BlockSpec(memory_space=pltpu.SMEM)] + [anywhere] * 6,
        out_specs=(pl.BlockSpec(memory_space=pl.ANY), vmem, vmem, vmem, vmem),
        scratch_shapes=[
            pltpu.VMEM((rows, width), F32),
            pltpu.VMEM((rows, width), F32),
            pltpu.VMEM((2, block, D), F32),
            pltpu.VMEM((2, block, D), F32),
            pltpu.VMEM((2, block, D), F32),
            pltpu.VMEM((2, rows, D), F32),
            pltpu.VMEM((keys, 3 * D), BF16),
            pltpu.VMEM((keys, 3 * D), BF16),
            pltpu.VMEM((2 * D, keys), BF16),
            pltpu.VMEM((pairs, 3 * D, 2 * rows), BF16),
            pltpu.VMEM((pairs, 3 * D, 2 * rows), BF16),
            pltpu.VMEM((pairs, 4 * rows, 2 * D), BF16),
            pltpu.VMEM((pairs, 4 * rows, 2 * D), BF16),
            pltpu.VMEM((pairs, keys, 2 * rows), F32),
            pltpu.VMEM((pairs, keys, 2 * rows), F32),
            pltpu.VMEM((pairs, 1, 2 * rows), F32),
            pltpu.VMEM((pairs, 1, 2 * rows), F32),
            pltpu.VMEM((pairs, 1, 2 * rows), F32),
            pltpu.VMEM((2, lead, 4 * rows), BF16),
            pltpu.VMEM((2, lead, 4 * rows), BF16),
            pltpu.VMEM((keys, D), F32),
            pltpu.VMEM((keys, D), F32),
            pltpu.VMEM((pairs, D, 2 * rows), F32),
            pltpu.VMEM((pairs, rows, 2 * D), F32),
            pltpu.VMEM((2, block, D), F32),
            pltpu.VMEM((2, block, D), F32),
        ]
        + [sems] * 4
        + [part_sems] * 4
        + [pltpu.SemaphoreType.DMA((n_head - 1, pairs))] * 2
        + [pltpu.SemaphoreType.DMA((pairs,)), pltpu.SemaphoreType.DMA((6,))],
        compiler_params=pltpu.CompilerParams(
            collective_id=0, has_side_effects=True, vmem_limit_bytes=63 * 1024 * 1024
        ),
    )(lengths, queries, prefix_keys, prefix_value_rows, response_keys, response_values, out_grad)
    return pl.pallas_call(
        settle,
        out_shape=tuple(shape(x.shape, x.dtype) for x in results),
        in_specs=[anywhere] * len(results),
        out_specs=(anywhere,) * len(results),
        scratch_shapes=[pltpu.SemaphoreType.DMA((len(results),))],
    )(*results)


def solution(mesh):
    sharded = P("seq", "head")
    return jax.shard_map(
        functools.partial(per_device, mesh.shape["seq"], mesh.shape["head"]),
        mesh=mesh,
        in_specs=(sharded,) * 6 + (P("seq"),),
        out_specs=(P(("seq", "head"), None),) + (sharded,) * 4,
        check_vma=False,
    )
```

```python
import functools
import math

import jax
import jax.numpy as jnp
from jax import lax
from jax.experimental import pallas as pl
from jax.experimental.pallas import tpu as pltpu
from jax.sharding import PartitionSpec as P

HEAD_SIZE = 128
WINDOW = 3
D = HEAD_SIZE
MESH = pl.DeviceIdType.MESH
F32, BF16 = jnp.float32, jnp.bfloat16
SUB = 128
UNROLL = 4


def split(x):
    hi = x.astype(BF16)
    lo = (x - hi.astype(F32)).astype(BF16)
    return hi, lo


def dot(a, b):
    return jnp.dot(a, b, preferred_element_type=F32)


def chunk_of(block):
    return (block // SUB + 1) // 2 * SUB


def kernel(
    n_seq, n_head,
    length_ref, q_hbm, pk_ref, pv_ref, rk_ref, rv_ref, g_hbm,
    gq_ref, gpk_ref, gpv_ref, grk_ref, grv_ref,
    q_ref, g_ref, kv0, kv1, kv2, kvr, kc, vc, kt, qt, gt, qr, gr, s_ref, dp_ref, m_ref, l_ref, d_ref,
    pcat, dcat, dk_acc, dv_acc, dqt, dqs, ry, rz,
    in_z_send, in_z_recv, in_y_send, in_y_recv,
    out_z_send, out_z_recv, out_y_send, out_y_recv,
    q_send, q_recv, q_local, load_sem,
):
    rows = q_hbm.shape[0]
    heads = q_hbm.shape[1] // D
    pairs = heads // 2
    block = pk_ref.shape[0]
    big = chunk_of(block)
    spans = ((0, big), (big, block - big))
    lead = block + rows
    off1, off2 = lead, lead + block
    factor = D ** (-0.5)
    seq = lax.axis_index("seq")
    head = lax.axis_index("head")
    even = lax.rem(seq, 2) == 0
    odd = jnp.logical_not(even)
    partner = seq + 1 - 2 * lax.rem(seq, 2)
    below = lax.rem(seq + n_seq - 2, n_seq)
    above = lax.rem(seq + 2, n_seq)

    barrier = pltpu.get_barrier_semaphore()
    for other in (partner, below, above):
        pl.semaphore_signal(barrier, inc=1, device_id=(other, head), device_id_type=MESH)
    for step in range(1, n_head):
        pl.semaphore_signal(
            barrier, inc=1, device_id=(seq, lax.rem(head + step, n_head)), device_id_type=MESH
        )
    loads = [
        pltpu.make_async_copy(src, dst, load_sem.at[i])
        for i, (src, dst) in enumerate(
            (
                (pk_ref, kv0.at[0]),
                (pv_ref, kv0.at[1]),
                (rk_ref, kvr.at[0]),
                (rv_ref, kvr.at[1]),
                (q_hbm, q_ref),
                (g_hbm, g_ref),
            )
        )
    ]
    for load in loads:
        load.start()
    pl.semaphore_wait(barrier, 3 + n_head - 1)

    def remote(src, dst, send, recv, to):
        return pltpu.make_async_remote_copy(
            src_ref=src, dst_ref=dst, send_sem=send, recv_sem=recv,
            device_id=to, device_id_type=MESH,
        )

    pieces = [(c, t) for c in range(2) for t in range(2)]
    own = (pk_ref, pv_ref)

    def at(c):
        return pl.ds(*spans[c])

    def in_z(c, t):
        return remote(own[t].at[at(c)], kv2.at[t, at(c)], in_z_send.at[c, t], in_z_recv.at[c, t], (below, head))

    def in_y_own(c, t):
        return remote(own[t].at[at(c)], kv1.at[t, at(c)], in_y_send.at[c, t], in_y_recv.at[c, t], (partner, head))

    def in_y_pass(c, t):
        return remote(kv2.at[t, at(c)], kv1.at[t, at(c)], in_y_send.at[c, t], in_y_recv.at[c, t], (partner, head))

    for c, t in pieces:
        in_z(c, t).start()

    @pl.when(odd)
    def _():
        for c, t in pieces:
            in_y_own(c, t).start()

    def place(keys, values, first, offset, size):
        for start in range(0, size, SUB):
            here = pl.ds(offset + start, SUB)
            k = keys[pl.ds(first + start, SUB), :]
            hi, lo = split(k)
            kc[here, 0:D] = hi
            kc[here, D : 2 * D] = lo
            kc[here, 2 * D : 3 * D] = hi
            hi, lo = split(k.T)
            kt[0:D, here] = hi
            kt[D : 2 * D, here] = lo
            hi, lo = split(values[pl.ds(first + start, SUB), :])
            vc[here, 0:D] = hi
            vc[here, D : 2 * D] = lo
            vc[here, 2 * D : 3 * D] = hi

    for load in loads[:4]:
        load.wait()
    place(kv0.at[0], kv0.at[1], 0, 0, block)
    place(kvr.at[0], kvr.at[1], 0, block, rows)
    for load in loads[4:]:
        load.wait()

    length = length_ref[0]
    token = lax.broadcasted_iota(jnp.int32, (rows, 1), 0)
    live = token < length
    for h in range(heads):
        cols = pl.ds(h * D, D)
        pair, half = h // 2, h % 2
        lanes = pl.ds(half * rows, rows)
        q = q_ref[:, cols]
        g = jnp.where(live, g_ref[:, cols], 0.0)
        for x, wide, tall, scale in (
            (q, qr, qt, factor * math.log2(math.e)),
            (g, gr, gt, 1.0),
        ):
            hi, lo = split((x * scale).T)
            tall[pair, 0:D, lanes] = hi
            tall[pair, D : 2 * D, lanes] = hi
            tall[pair, 2 * D : 3 * D, lanes] = lo
            hi, lo = split(x * factor) if wide is qr else split(x)
            for copy in range(2):
                at_rows = pl.ds(copy * 2 * rows + half * rows, rows)
                wide[pair, at_rows, 0:D] = hi
                wide[pair, at_rows, D : 2 * D] = lo

    def scores(offset, size, first):
        def products(pair):
            s = dot(kc[pl.ds(offset, size), :], qt[pair])
            if first:
                slot = lax.broadcasted_iota(jnp.int32, (rows, 2 * rows), 0)
                lane = lax.broadcasted_iota(jnp.int32, (rows, 2 * rows), 1)
                query = jnp.where(lane >= rows, lane - rows, lane)
                visible = (slot <= query) & (slot < length)
                s_ref[pair, pl.ds(offset, block), :] = s[:block]
                s_ref[pair, pl.ds(offset + block, rows), :] = jnp.where(visible, s[block:], -1e30)
            else:
                s_ref[pair, pl.ds(offset, size), :] = s
            dp_ref[pair, pl.ds(offset, size), :] = dot(vc[pl.ds(offset, size), :], gt[pair])

        def sums(pair):
            top = None
            for start in range(0, size, SUB):
                part = jnp.max(
                    s_ref[pair, pl.ds(offset + start, SUB), :].reshape(SUB // 8, 8, 2 * rows), axis=0
                )
                top = part if top is None else jnp.maximum(top, part)
            top = jnp.max(top, axis=0, keepdims=True)
            total = jnp.zeros((8, 2 * rows), F32)
            dsum = jnp.zeros((8, 2 * rows), F32)
            for start in range(0, size, SUB):
                here = pl.ds(offset + start, SUB)
                e = jnp.exp2(s_ref[pair, here, :] - top)
                total = total + jnp.sum(e.reshape(SUB // 8, 8, 2 * rows), axis=0)
                dsum = dsum + jnp.sum((e * dp_ref[pair, here, :]).reshape(SUB // 8, 8, 2 * rows), axis=0)
            total = jnp.sum(total, axis=0, keepdims=True)
            dsum = jnp.sum(dsum, axis=0, keepdims=True)
            if first:
                m_ref[pair] = top
                l_ref[pair] = total
                d_ref[pair] = dsum
            else:
                newest = jnp.maximum(m_ref[pair], top)
                fade, add = jnp.exp2(m_ref[pair] - newest), jnp.exp2(top - newest)
                m_ref[pair] = newest
                l_ref[pair] = l_ref[pair] * fade + total * add
                d_ref[pair] = d_ref[pair] * fade + dsum * add

        def body(i, carry):
            for j in range(UNROLL):
                products(i * UNROLL + j)
                if j:
                    sums(i * UNROLL + j - 1)
            sums(i * UNROLL + UNROLL - 1)
            return carry

        lax.fori_loop(0, pairs // UNROLL, body, 0)

    def grads(offset, size, first, begin=0, end=None, then=None):
        keys = pl.ds(offset, size)
        if begin == 0:
            dk_acc[keys, :] = jnp.zeros((size, D), F32)
            dv_acc[keys, :] = jnp.zeros((size, D), F32)
        some = pl.ds(0, size)

        def weights(pair, slot):
            shift, mean = m_ref[pair], d_ref[pair]
            for start in range(0, size, SUB):
                here = pl.ds(offset + start, SUB)
                p = jnp.exp2(s_ref[pair, here, :] - shift)
                ds = p * (dp_ref[pair, here, :] - mean)
                to = pl.ds(start, SUB)
                hi, lo = split(p)
                pcat[slot, to, 0 : 2 * rows] = hi
                pcat[slot, to, 2 * rows :] = lo
                hi, lo = split(ds)
                dcat[slot, to, 0 : 2 * rows] = hi
                dcat[slot, to, 2 * rows :] = lo

        def products(pair, slot):
            dv = dot(pcat[slot, some, :], gr[pair])
            dv_acc[keys, :] += dv[:, :D] + dv[:, D:]
            dk = dot(dcat[slot, some, :], qr[pair])
            dk_acc[keys, :] += dk[:, :D] + dk[:, D:]
            high = dot(kt[:, keys], dcat[slot, some, 0 : 2 * rows])
            dq = high[:D] + high[D:] + dot(kt[0:D, keys], dcat[slot, some, 2 * rows :])
            if first:
                dqt[pair] = dq
            elif then is None:
                dqt[pair] += dq
            else:
                then(pair, dqt[pair] + dq)

        def body(i, carry):
            weights(2 * i, 0)
            weights(2 * i + 1, 1)
            products(2 * i, 0)
            products(2 * i + 1, 1)
            return carry

        lax.fori_loop(begin // 2, (pairs if end is None else end) // 2, body, 0)

    scores(0, lead, True)
    for c in range(2):
        for t in range(2):
            in_z(c, t).wait_recv()

            @pl.when(even)
            def _():
                in_y_pass(c, t).start()

        place(kv2.at[0], kv2.at[1], spans[c][0], off2 + spans[c][0], spans[c][1])
        scores(off2 + spans[c][0], spans[c][1], False)
        for t in range(2):
            in_y_own(c, t).wait_recv()
        place(kv1.at[0], kv1.at[1], spans[c][0], off1 + spans[c][0], spans[c][1])
        scores(off1 + spans[c][0], spans[c][1], False)

    def finish(pair, carry):
        l = l_ref[pair]
        d_ref[pair] = d_ref[pair] / l
        m_ref[pair] = m_ref[pair] + jnp.log2(l)
        return carry

    lax.fori_loop(0, pairs, finish, 0)

    acc = (dk_acc, dv_acc)
    parts = block // SUB
    order = list(range(spans[1][0] // SUB, parts)) + list(range(spans[1][0] // SUB))
    split_at = spans[1][1] // SUB

    def out_y(i, t):
        return remote(
            acc[t].at[pl.ds(off1 + i * SUB, SUB)], ry.at[t, pl.ds(i * SUB, SUB)],
            out_y_send.at[i, t], out_y_recv.at[i, t], (partner, head),
        )

    def out_z(i, t):
        return remote(
            acc[t].at[pl.ds(off2 + i * SUB, SUB)], rz.at[t, pl.ds(i * SUB, SUB)],
            out_z_send.at[i, t], out_z_recv.at[i, t], (above, head),
        )

    def send_y(some):
        for i in some:
            for t in range(2):
                out_y(i, t).start()

    def send_z_odd(some):
        @pl.when(odd)
        def _():
            for i in some:
                for t in range(2):
                    out_z(i, t).start()

    def join(some):
        for i in some:
            for t in range(2):
                out_y(i, t).wait_recv()

            @pl.when(even)
            def _():
                for t in range(2):
                    acc[t][pl.ds(off2 + i * SUB, SUB), :] += ry[t, pl.ds(i * SUB, SUB), :]
                for t in range(2):
                    out_z(i, t).start()

    width = heads * D
    share = rows // n_head

    def to_peer(step, pair):
        other = lax.rem(head + step, n_head)
        return remote(
            dqs.at[pair, pl.ds(other * share, share), :],
            gq_ref.at[:, pl.ds(pl.multiple_of(head * width + pair * 2 * D, D), 2 * D)],
            q_send.at[step - 1, pair], q_recv.at[step - 1, pair], (seq, other),
        )

    def keep(pair):
        return pltpu.make_async_copy(
            dqs.at[pair, pl.ds(head * share, share), :],
            gq_ref.at[:, pl.ds(pl.multiple_of(head * width + pair * 2 * D, D), 2 * D)],
            q_local.at[pair],
        )

    def stage(pair, dq):
        for half in range(2):
            dqs[pair, :, half * D : (half + 1) * D] = dq[:, half * rows : (half + 1) * rows].T * factor
        for step in range(1, n_head):
            to_peer(step, pair).start()
        keep(pair).start()

    last, front = spans[1], spans[0]
    grads(off1 + last[0], last[1], True)
    send_y(order[:split_at])
    grads(off2 + last[0], last[1], False)
    send_z_odd(order[:split_at])
    grads(off1 + front[0], front[1], False)
    send_y(order[split_at:])
    join(order[:1])
    grads(off2 + front[0], front[1], False)
    send_z_odd(order[split_at:])
    join(order[1:split_at])
    middle = pairs // 4 * 2
    grads(0, lead, False, 0, middle, stage)
    join(order[split_at : split_at + 1])
    grads(0, lead, False, middle, pairs, stage)
    grk_ref[...] = dk_acc[pl.ds(block, rows), :]
    grv_ref[...] = dv_acc[pl.ds(block, rows), :]
    join(order[split_at + 1 :])

    @pl.when(odd)
    def _():
        for t in range(2):
            acc[t][pl.ds(0, block), :] += ry[t]

    out = (gpk_ref, gpv_ref)
    for i in order:
        for t in range(2):
            here = pl.ds(i * SUB, SUB)
            out_z(i, t).wait_recv()
            out[t][here, :] = acc[t][here, :] + rz[t, here, :]

    for pair in range(pairs):
        keep(pair).wait()
        for step in range(1, n_head):
            to_peer(step, pair).wait()
    for c, t in pieces:
        in_z(c, t).wait_send()
        in_y_own(c, t).wait_send()
    for i in order:
        for t in range(2):
            out_y(i, t).wait_send()
            out_z(i, t).wait_send()


def settle(*refs):
    count = (len(refs) - 2) // 3
    load_sem, store_sem = refs[-2:]
    held = refs[2 * count : 3 * count]
    loads = [
        pltpu.make_async_copy(refs[i], held[i], load_sem.at[i]) for i in range(count)
    ]
    stores = [
        pltpu.make_async_copy(held[i], refs[count + i], store_sem.at[i]) for i in range(count)
    ]
    for load in loads:
        load.start()
    for load, store in zip(loads, stores):
        load.wait()
        store.start()
    for store in stores:
        store.wait()


def per_device(n_seq, n_head, queries, prefix_keys, prefix_value_rows, response_keys, response_values, out_grad, lengths):
    rows, width = queries.shape
    block = prefix_keys.shape[0]
    assert prefix_keys.shape[1] == D
    heads = width // D
    pairs = heads // 2
    keys = WINDOW * block + rows
    lead = block + rows
    vmem = pl.BlockSpec(memory_space=pltpu.VMEM)
    anywhere = pl.BlockSpec(memory_space=pl.ANY)
    sems = pltpu.SemaphoreType.DMA((2, 2))
    part_sems = pltpu.SemaphoreType.DMA((block // SUB, 2))
    shape = jax.ShapeDtypeStruct
    results = pl.pallas_call(
        functools.partial(kernel, n_seq, n_head),
        out_shape=(
            shape((rows // n_head, width * n_head), F32),
            shape((block, D), F32),
            shape((block, D), F32),
            shape((rows, D), F32),
            shape((rows, D), F32),
        ),
        in_specs=[pl.BlockSpec(memory_space=pltpu.SMEM)] + [anywhere] * 6,
        out_specs=(pl.BlockSpec(memory_space=pl.ANY), vmem, vmem, vmem, vmem),
        scratch_shapes=[
            pltpu.VMEM((rows, width), F32),
            pltpu.VMEM((rows, width), F32),
            pltpu.VMEM((2, block, D), F32),
            pltpu.VMEM((2, block, D), F32),
            pltpu.VMEM((2, block, D), F32),
            pltpu.VMEM((2, rows, D), F32),
            pltpu.VMEM((keys, 3 * D), BF16),
            pltpu.VMEM((keys, 3 * D), BF16),
            pltpu.VMEM((2 * D, keys), BF16),
            pltpu.VMEM((pairs, 3 * D, 2 * rows), BF16),
            pltpu.VMEM((pairs, 3 * D, 2 * rows), BF16),
            pltpu.VMEM((pairs, 4 * rows, 2 * D), BF16),
            pltpu.VMEM((pairs, 4 * rows, 2 * D), BF16),
            pltpu.VMEM((pairs, keys, 2 * rows), F32),
            pltpu.VMEM((pairs, keys, 2 * rows), F32),
            pltpu.VMEM((pairs, 1, 2 * rows), F32),
            pltpu.VMEM((pairs, 1, 2 * rows), F32),
            pltpu.VMEM((pairs, 1, 2 * rows), F32),
            pltpu.VMEM((2, lead, 4 * rows), BF16),
            pltpu.VMEM((2, lead, 4 * rows), BF16),
            pltpu.VMEM((keys, D), F32),
            pltpu.VMEM((keys, D), F32),
            pltpu.VMEM((pairs, D, 2 * rows), F32),
            pltpu.VMEM((pairs, rows, 2 * D), F32),
            pltpu.VMEM((2, block, D), F32),
            pltpu.VMEM((2, block, D), F32),
        ]
        + [sems] * 4
        + [part_sems] * 4
        + [pltpu.SemaphoreType.DMA((n_head - 1, pairs))] * 2
        + [pltpu.SemaphoreType.DMA((pairs,)), pltpu.SemaphoreType.DMA((6,))],
        compiler_params=pltpu.CompilerParams(
            collective_id=0, has_side_effects=True, vmem_limit_bytes=63 * 1024 * 1024
        ),
    )(lengths, queries, prefix_keys, prefix_value_rows, response_keys, response_values, out_grad)
    return pl.pallas_call(
        settle,
        out_shape=tuple(shape(x.shape, x.dtype) for x in results),
        in_specs=[anywhere] * len(results),
        out_specs=(anywhere,) * len(results),
        scratch_shapes=[pltpu.VMEM(x.shape, x.dtype) for x in results]
        + [pltpu.SemaphoreType.DMA((len(results),))] * 2,
    )(*results)


def solution(mesh):
    sharded = P("seq", "head")
    return jax.shard_map(
        functools.partial(per_device, mesh.shape["seq"], mesh.shape["head"]),
        mesh=mesh,
        in_specs=(sharded,) * 6 + (P("seq"),),
        out_specs=(P(("seq", "head"), None),) + (sharded,) * 4,
        check_vma=False,
    )
```
